32 devices in a mesh: dp: 1, tp: 32 (over x, y, z, core).
Axes of the slice: x: 2, y: 2, z: 4, core: 2. Of those that a mesh axis runs over, the one named last changes fastest.
Arguments:
- x: bfloat16 [2048, 8192], P('dp')
- w_gate: bfloat16 [8192, 28672], P(None, 'tp')
- w_up: bfloat16 [8192, 28672], P(None, 'tp')
- w_down: bfloat16 [28672, 8192], P('tp')
Outputs:
- output: bfloat16 [2048, 8192], P('dp')
All inputs are finite; a program needn't handle non-finite values.
Results may differ from the reference program's by a relative error of at most 0.016.
Values are sent between devices in bfloat16 or wider.
A program may use at most 2 GiB of HBM per device.

```python
import jax
import jax.numpy as jnp

ROWS = 2048
D = 8192
FF = 28672


def setup_inputs(seed: int = 0, part: int = 0) -> dict:
    kx, kg, ku, kd = jax.random.split(jax.random.key(seed), 4)
    drawn = {
        "x": jax.random.normal(jax.random.fold_in(kx, part), (ROWS, D), jnp.float32),
        "w_gate": jax.random.normal(kg, (D, FF), jnp.float32) * D**-0.5,
        "w_up": jax.random.normal(ku, (D, FF), jnp.float32) * D**-0.5,
        "w_down": jax.random.normal(kd, (FF, D), jnp.float32) * FF**-0.5,
    }
    return {k: v.astype(jnp.bfloat16) for k, v in drawn.items()}


def reference(x, w_gate, w_up, w_down):
    gate = jnp.dot(x, w_gate, preferred_element_type=jnp.float32)
    up = jnp.dot(x, w_up, preferred_element_type=jnp.float32)
    hidden = (jax.nn.silu(gate) * up).astype(jnp.bfloat16)
    return jnp.dot(hidden, w_down, preferred_element_type=jnp.float32).astype(jnp.bfloat16)
```

```python
import functools

import jax
import jax.numpy as jnp
from jax import lax
from jax.experimental import pallas as pl
from jax.experimental.pallas import tpu as pltpu
from jax.sharding import PartitionSpec as P

MESH = pl.DeviceIdType.MESH
F32, BF16 = jnp.float32, jnp.bfloat16
ROWS, D, F = 2048, 8192, 896
RB, KB, CB = 512, 1024, 1024
NK, NC = D // KB, D // CB
TILES = (ROWS // RB) * NC
SLOTS = 16
ZSLOTS = 8
LAG = (1, 3, 5, 7, 9, 11, 13, 15, 17, 19, 21, 22)
STEPS = NK + TILES + 2 + (max(LAG) + 1) // 2


def kernel(
    x, wg, wu, wd, out,
    x_buf, gu_buf, wd_buf, acc, hid,
    own, d_send, d_recv, f_send, f_keep, f_recv, zacc, z_send, z_recv, l_send, l_recv, y_buf,
    load_sem, ds_sem, dr_sem, fs_sem, fr_sem, zs_sem, zr_sem, ls_sem, lr_sem, yl_sem,
    als_sem, alr_sem, azs_sem, azr_sem, afs_sem, afr_sem, ads_sem, adr_sem,
):
    me = lax.axis_index("tp")
    core = lax.rem(me, 2)
    z = lax.rem(lax.div(me, 2), 4)
    yy = lax.rem(lax.div(me, 8), 2)
    xx = lax.div(me, 16)
    peer_core = me + 1 - 2 * core
    peer_x = me + 16 - 32 * xx
    peer_y = me + 8 - 16 * yy
    toward = (me + 2, me - 2)
    first, last = (xx, yy), (yy, xx)
    first_peer, last_peer = (peer_x, peer_y), (peer_y, peer_x)

    barrier = pltpu.get_barrier_semaphore()

    def greet(device):
        pl.semaphore_signal(barrier, inc=1, device_id={"tp": device}, device_id_type=MESH)

    greet(peer_core)
    greet(peer_x)
    greet(peer_y)

    @pl.when(z < 3)
    def _():
        greet(me + 2)

    @pl.when(z > 0)
    def _():
        greet(me - 2)

    pl.semaphore_wait(barrier, 3 + jnp.where(z < 3, 1, 0) + jnp.where(z > 0, 1, 0))

    def remote(src, dst, send_sem, recv_sem, device):
        return pltpu.make_async_remote_copy(
            src_ref=src, dst_ref=dst, send_sem=send_sem, recv_sem=recv_sem,
            device_id={"tp": device}, device_id_type=MESH,
        )

    def block(c, row, rows):
        start = pl.multiple_of(lax.div(c, NC) * RB + row, 8)
        return out.at[pl.ds(start, rows), pl.ds(pl.multiple_of(lax.rem(c, NC) * CB, CB), CB)]

    def d_copy(c):
        return remote(d_send.at[c % 2], d_recv.at[c % SLOTS], ds_sem.at[c % 2], dr_sem.at[c % SLOTS], peer_core)

    def f_copy(c, k):
        return remote(
            f_send.at[c % 2, k], f_recv.at[c % SLOTS, k], fs_sem.at[k, c % 2], fr_sem.at[k, c % SLOTS], first_peer[k]
        )

    def z_copy(c, way, s):
        return remote(
            z_send.at[way, s - 1, c % 2], z_recv.at[way, s - 1, c % SLOTS],
            zs_sem.at[way * 3 + s - 1, c % 2], zr_sem.at[way * 3 + s - 1, c % SLOTS], toward[way],
        )

    def l_copy(c, k):
        return remote(
            l_send.at[c % 2, k], l_recv.at[c % SLOTS, k], ls_sem.at[k, c % 2], lr_sem.at[k, c % SLOTS], last_peer[k]
        )

    def y_local(c, k):
        rows = block(c, core * 256 + k * 128 + first[k] * 64 + z * 16 + last[k] * 8, 8)
        return pltpu.make_async_copy(y_buf.at[c % 2, k], rows, yl_sem.at[k, c % 2])

    def al_copy(c, k, half):
        rows = block(c, core * 256 + k * 128 + first[k] * 64 + z * 16 + half * 8, 8)
        return remote(y_buf.at[c % 2, k], rows, als_sem.at[k, c % 2], alr_sem.at[k, c % SLOTS], last_peer[k])

    def az_copy(c, way, s, k, piece):
        rows = block(c, core * 256 + k * 128 + first[k] * 64 + piece * 16, 16)
        i = (way * 3 + s - 1) * 2 + k
        return remote(rows, rows, azs_sem.at[i, c % 2], azr_sem.at[i, c % SLOTS], toward[way])

    def af_copy(c, k, half):
        rows = block(c, core * 256 + k * 128 + half * 64, 64)
        return remote(rows, rows, afs_sem.at[k, c % 2], afr_sem.at[k, c % SLOTS], first_peer[k])

    def ad_copy(c, half):
        rows = block(c, half * 256, 256)
        return remote(rows, rows, ads_sem.at[c % 2], adr_sem.at[c % SLOTS], peer_core)

    def z_piece(way, s):
        piece = 4 - s + z if way == 0 else z + s - 4
        ok = (z <= 2) & (piece <= 3) if way == 0 else (z >= 1) & (piece >= 0)
        return piece, ok

    def z_got(way, s):
        piece = 3 - s + z if way == 0 else z + s - 3
        ok = (z >= 1) & (piece <= 3) if way == 0 else (z <= 2) & (piece >= 0)
        return piece, ok

    def z_go(c, s):
        for way in range(2):
            piece, ok = z_piece(way, s)

            @pl.when(ok)
            def _():
                z_send[way, s - 1, c % 2] = zacc[c % ZSLOTS, piece].astype(BF16)
                z_copy(c, way, s).start()

    def z_free(c, s):
        for way in range(2):
            piece, ok = z_piece(way, s)

            @pl.when(ok)
            def _():
                z_copy(c, way, s).wait_send()

    def r0(c):
        d_copy(c).wait_recv()
        for k in range(2):
            rows = pl.ds(pl.multiple_of(k * 128 + (1 - first[k]) * 64, 64), 64)
            f_send[c % 2, k] = (own[c % 2, rows] + d_recv[c % SLOTS, rows].astype(F32)).astype(BF16)
            f_copy(c, k).start()
        for k in range(2):
            rows = pl.ds(pl.multiple_of(k * 128 + first[k] * 64, 64), 64)
            f_keep[c % 2, k] = own[c % 2, rows] + d_recv[c % SLOTS, rows].astype(F32)

    def r0_free(c):
        for k in range(2):
            f_copy(c, k).wait_send()

    def r1(c):
        for k in range(2):
            f_copy(c, k).wait_recv()
            for j in range(4):
                rows = pl.ds(j * 16, 16)
                zacc[c % ZSLOTS, j, k] = f_keep[c % 2, k, rows] + f_recv[c % SLOTS, k, rows].astype(F32)
        z_go(c, 1)

    def rz(s):
        def stage(c):
            for way in range(2):
                piece, ok = z_got(way, s)

                @pl.when(ok)
                def _():
                    z_copy(c, way, s).wait_recv()
                    zacc[c % ZSLOTS, piece] = (
                        zacc[c % ZSLOTS, piece] + z_recv[way, s - 1, c % SLOTS].astype(F32)
                    )

            if s < 3:
                z_go(c, s + 1)
                return
            for k in range(2):
                rows = pl.ds(pl.multiple_of((1 - last[k]) * 8, 8), 8)
                l_send[c % 2, k] = zacc[c % ZSLOTS, z, k, rows].astype(BF16)
                l_copy(c, k).start()

        return stage

    def l_free(c):
        for k in range(2):
            l_copy(c, k).wait_send()

    def r5(c):
        for k in range(2):
            l_copy(c, k).wait_recv()
            rows = pl.ds(pl.multiple_of(last[k] * 8, 8), 8)
            y_buf[c % 2, k] = (zacc[c % ZSLOTS, z, k, rows] + l_recv[c % SLOTS, k].astype(F32)).astype(BF16)
            y_local(c, k).start()
            al_copy(c, k, last[k]).start()

    def r5_free(c):
        for k in range(2):
            al_copy(c, k, last[k]).wait_send()

    def az_piece(way, s):
        piece = z - (s - 1) if way == 0 else z + (s - 1)
        ok = (z <= 2) & (piece >= 0) if way == 0 else (z >= 1) & (piece <= 3)
        return piece, ok

    def az_go(c, s):
        for way in range(2):
            piece, ok = az_piece(way, s)

            @pl.when(ok)
            def _():
                for k in range(2):
                    az_copy(c, way, s, k, piece).start()

    def az_free(c, s):
        for way in range(2):
            piece, ok = az_piece(way, s)

            @pl.when(ok)
            def _():
                for k in range(2):
                    az_copy(c, way, s, k, piece).wait_send()

    def a0(c):
        for k in range(2):
            y_local(c, k).wait()
            al_copy(c, k, 1 - last[k]).wait_recv()
        az_go(c, 1)

    def az(s):
        def stage(c):
            for way in range(2):
                piece = z - s if way == 0 else z + s
                ok = piece >= 0 if way == 0 else piece <= 3

                @pl.when(ok)
                def _():
                    for k in range(2):
                        az_copy(c, way, s, k, piece).wait_recv()

            if s < 3:
                az_go(c, s + 1)
                return
            for k in range(2):
                af_copy(c, k, first[k]).start()

        return stage

    def af_free(c):
        for k in range(2):
            af_copy(c, k, first[k]).wait_send()

    def a4(c):
        for k in range(2):
            af_copy(c, k, 1 - first[k]).wait_recv()
        ad_copy(c, core).start()

    def a4_free(c):
        ad_copy(c, core).wait_send()

    def a5(c):
        ad_copy(c, 1 - core).wait_recv()

    stages = (
        (r0, r0_free),
        (r1, lambda c: z_free(c, 1)),
        (rz(1), lambda c: z_free(c, 2)),
        (rz(2), lambda c: z_free(c, 3)),
        (rz(3), l_free),
        (r5, r5_free),
        (a0, lambda c: az_free(c, 1)),
        (az(1), lambda c: az_free(c, 2)),
        (az(2), lambda c: az_free(c, 3)),
        (az(3), af_free),
        (a4, a4_free),
        (a5, None),
    )

    def comm(t, part):
        for lag, (stage, free) in zip(LAG, stages):
            if lag % 2 != part:
                continue
            c = t - NK - lag // 2
            if free is not None:

                @pl.when((c >= 2) & (c < TILES + 2))
                def _():
                    free(c - 2)

            @pl.when((c >= 0) & (c < TILES))
            def _():
                stage(c)

    def loads(t):
        p = t % 2
        rows = pl.ds(pl.multiple_of(lax.div(t, NK) * RB, RB), RB)
        deep = pl.ds(pl.multiple_of(lax.rem(t, NK) * KB, KB), KB)
        cols = pl.ds(pl.multiple_of(lax.rem(t, NC) * CB, CB), CB)
        up = (
            pltpu.make_async_copy(x.at[rows, deep], x_buf.at[p], load_sem.at[p, 0]),
            pltpu.make_async_copy(wg.at[deep], gu_buf.at[p, :, pl.ds(0, F)], load_sem.at[p, 1]),
            pltpu.make_async_copy(wu.at[deep], gu_buf.at[p, :, pl.ds(F, F)], load_sem.at[p, 2]),
        )
        down = pltpu.make_async_copy(wd.at[:, cols], wd_buf.at[p], load_sem.at[p, 3])
        return up, down

    def fetch(t):
        up, down = loads(t)

        @pl.when(t < TILES)
        def _():
            for copy in up:
                copy.start()

        @pl.when((t >= NK) & (t < NK + TILES))
        def _():
            down.start()

    acc[...] = jnp.zeros_like(acc)
    fetch(jnp.int32(0))

    def step(t, _):
        fetch(t + 1)
        up, down = loads(t)
        p = t % 2
        c = t - NK

        @pl.when((c >= 2) & (c < TILES + 2))
        def _():
            d_copy(c - 2).wait_send()

        @pl.when((c >= 0) & (c < TILES))
        def _():
            down.wait()
            w = wd_buf[p]
            d_send[c % 2] = jnp.dot(hid[1 - core], w, preferred_element_type=F32).astype(BF16)
            d_copy(c).start()
            own[c % 2] = jnp.dot(hid[core], w, preferred_element_type=F32)

        comm(t, 0)

        @pl.when(t < TILES)
        def _():
            for copy in up:
                copy.wait()
            acc[...] += jnp.dot(x_buf[p], gu_buf[p], preferred_element_type=F32)

            @pl.when(t % NK == NK - 1)
            def _():
                for half in range(2):
                    rows = pl.ds(half * 256, 256)
                    gate = acc[rows, pl.ds(0, F)]
                    hid[half] = (gate * jax.nn.sigmoid(gate) * acc[rows, pl.ds(F, F)]).astype(BF16)
                acc[...] = jnp.zeros_like(acc)

        comm(t, 1)
        return 0

    lax.fori_loop(0, STEPS, step, 0)


def block_of(x, wg, wu, wd):
    any_space = pl.BlockSpec(memory_space=pl.ANY)
    dma = pltpu.SemaphoreType.DMA
    return pl.pallas_call(
        kernel,
        out_shape=jax.ShapeDtypeStruct((ROWS, D), BF16),
        in_specs=[any_space] * 4,
        out_specs=any_space,
        scratch_shapes=[
            pltpu.VMEM((2, RB, KB), BF16),
            pltpu.VMEM((2, KB, 2 * F), BF16),
            pltpu.VMEM((2, F, CB), BF16),
            pltpu.VMEM((RB, 2 * F), F32),
            pltpu.VMEM((2, RB // 2, F), BF16),
            pltpu.VMEM((2, 256, CB), F32),
            pltpu.VMEM((2, 256, CB), BF16),
            pltpu.VMEM((SLOTS, 256, CB), BF16),
            pltpu.VMEM((2, 2, 64, CB), BF16),
            pltpu.VMEM((2, 2, 64, CB), F32),
            pltpu.VMEM((SLOTS, 2, 64, CB), BF16),
            pltpu.VMEM((ZSLOTS, 4, 2, 16, CB), F32),
            pltpu.VMEM((2, 3, 2, 2, 16, CB), BF16),
            pltpu.VMEM((2, 3, SLOTS, 2, 16, CB), BF16),
            pltpu.VMEM((2, 2, 8, CB), BF16),
            pltpu.VMEM((SLOTS, 2, 8, CB), BF16),
            pltpu.VMEM((2, 2, 8, CB), BF16),
            dma((2, 4)),
            dma((2,)), dma((SLOTS,)),
            dma((2, 2)), dma((2, SLOTS)),
            dma((6, 2)), dma((6, SLOTS)),
            dma((2, 2)), dma((2, SLOTS)),
            dma((2, 2)),
            dma((2, 2)), dma((2, SLOTS)),
            dma((12, 2)), dma((12, SLOTS)),
            dma((2, 2)), dma((2, SLOTS)),
            dma((2,)), dma((SLOTS,)),
        ],
        compiler_params=pltpu.CompilerParams(
            collective_id=0, has_side_effects=True, vmem_limit_bytes=66_000_000
        ),
    )(x, wg, wu, wd)


def solution(mesh):
    return jax.shard_map(
        block_of,
        mesh=mesh,
        in_specs=(P("dp", None), P(None, "tp"), P(None, "tp"), P("tp", None)),
        out_specs=P("dp", None),
        check_vma=False,
    )
```

```python
import jax
import jax.numpy as jnp
from jax import lax
from jax.experimental import pallas as pl
from jax.experimental.pallas import tpu as pltpu
from jax.sharding import PartitionSpec as P

MESH = pl.DeviceIdType.MESH
F32, BF16 = jnp.float32, jnp.bfloat16
ROWS, D, F = 2048, 8192, 896
RB, KB, CB = 256, 1024, 1024
NK, NC = D // KB, D // CB
TILES = (ROWS // RB) * NC
SLOTS = 24
SENDS = 4
ZSLOTS = 6
HBM_ROWS = 512
JOIN = 4
HBM_TILES = HBM_ROWS // RB * NC
HALF, QUARTER, EIGHTH, PIECE = RB // 2, RB // 4, RB // 8, RB // 32
LAG = (2, 6, 9, 11, 14, 18, 21, 24, 26, 34, 36)
STEPS = NK + TILES + SENDS + max(LAG) // 2 + 1


def kernel(
    x, wg, wu, wd, out_h, out_v,
    x_buf, gu_buf, wd_buf, acc, hid, term,
    own, d_send, d_recv, f_send, f_keep, f_recv, zacc, z_send, z_recv, l_send, l_recv, y_buf,
    load_sem, ds_sem, dr_sem, fs_sem, fr_sem, zs_sem, zr_sem, ls_sem, lr_sem, yl_sem,
    azs_sem, azr_sem, afs_sem, afr_sem, ads_sem, adr_sem,
):
    me = lax.axis_index("tp")
    core = lax.rem(me, 2)
    z = lax.rem(lax.div(me, 2), 4)
    yy = lax.rem(lax.div(me, 8), 2)
    xx = lax.div(me, 16)
    peer_core = me + 1 - 2 * core
    peer_x = me + 16 - 32 * xx
    peer_y = me + 8 - 16 * yy
    toward = (me + 2, me - 2)
    first = (xx, yy)
    first_peer, last_peer = (peer_x, peer_y), (peer_y, peer_x)

    barrier = pltpu.get_barrier_semaphore()

    def greet(device):
        pl.semaphore_signal(barrier, inc=1, device_id={"tp": device}, device_id_type=MESH)

    greet(peer_core)
    greet(peer_x)
    greet(peer_y)

    @pl.when(z < 3)
    def _():
        greet(me + 2)

    @pl.when(z > 0)
    def _():
        greet(me - 2)

    pl.semaphore_wait(barrier, 3 + jnp.where(z < 3, 1, 0) + jnp.where(z > 0, 1, 0))

    def remote(src, dst, send_sem, recv_sem, device):
        return pltpu.make_async_remote_copy(
            src_ref=src, dst_ref=dst, send_sem=send_sem, recv_sem=recv_sem,
            device_id={"tp": device}, device_id_type=MESH,
        )

    def block(c, row, rows, place):
        ref, base = ((out_h, 0), (out_v, HBM_ROWS))[place]
        start = pl.multiple_of(lax.div(c, NC) * RB - base + row, PIECE)
        return ref.at[pl.ds(start, rows), pl.ds(pl.multiple_of(lax.rem(c, NC) * CB, CB), CB)]

    def d_copy(c):
        return remote(d_send.at[c % SENDS], d_recv.at[c % SLOTS], ds_sem.at[c % SENDS], dr_sem.at[c % SLOTS], peer_core)

    def f_copy(c, k):
        return remote(
            f_send.at[c % SENDS, k], f_recv.at[c % SLOTS, k], fs_sem.at[k, c % SENDS], fr_sem.at[k, c % SLOTS], first_peer[k]
        )

    def z_copy(c, way, s):
        return remote(
            z_send.at[way, s - 1, c % SENDS], z_recv.at[way, s - 1, c % SLOTS],
            zs_sem.at[way * 3 + s - 1, c % SENDS], zr_sem.at[way * 3 + s - 1, c % SLOTS], toward[way],
        )

    def l_copy(c, k):
        return remote(
            l_send.at[c % SENDS, k], l_recv.at[c % SLOTS, k], ls_sem.at[k, c % SENDS], lr_sem.at[k, c % SLOTS], last_peer[k]
        )

    def piece_of(c, k, piece, place):
        return block(c, core * HALF + k * QUARTER + first[k] * EIGHTH + piece * PIECE, PIECE, place)

    def y_local(c, k):
        return pltpu.make_async_copy(y_buf.at[c % SENDS, k], piece_of(c, k, z, 0), yl_sem.at[k, c % SENDS])

    def az_copy(c, way, s, k, piece, place):
        rows = piece_of(c, k, piece, place)
        i = (way * 3 + s - 1) * 2 + k
        src = y_buf.at[c % SENDS, k] if s == 1 else rows
        return remote(src, rows, azs_sem.at[i, c % SENDS], azr_sem.at[i, c % SLOTS], toward[way])

    def af_copy(c, k, half, place):
        rows = block(c, core * HALF + k * QUARTER + half * EIGHTH, EIGHTH, place)
        return remote(rows, rows, afs_sem.at[k, c % SENDS], afr_sem.at[k, c % SLOTS], first_peer[k])

    def ad_copy(c, half, place):
        rows = block(c, half * HALF, HALF, place)
        return remote(rows, rows, ads_sem.at[c % SENDS], adr_sem.at[c % SLOTS], peer_core)

    def z_piece(way, s):
        piece = 4 - s + z if way == 0 else z + s - 4
        ok = (z <= 2) & (piece <= 3) if way == 0 else (z >= 1) & (piece >= 0)
        return piece, ok

    def z_got(way, s):
        piece = 3 - s + z if way == 0 else z + s - 3
        ok = (z >= 1) & (piece <= 3) if way == 0 else (z <= 2) & (piece >= 0)
        return piece, ok

    def z_go(c, s):
        for way in range(2):
            piece, ok = z_piece(way, s)

            @pl.when(ok)
            def _():
                z_send[way, s - 1, c % SENDS] = zacc[c % ZSLOTS, piece].astype(BF16)
                z_copy(c, way, s).start()

    def z_free(s):
        def free(c, place):
            for way in range(2):
                piece, ok = z_piece(way, s)

                @pl.when(ok)
                def _():
                    z_copy(c, way, s).wait_send()

        return free

    def r0(c, place):
        d_copy(c).wait_recv()
        for k in range(2):
            rows = pl.ds(pl.multiple_of(k * QUARTER + (1 - first[k]) * EIGHTH, EIGHTH), EIGHTH)
            f_send[c % SENDS, k] = (own[c % 3, rows] + d_recv[c % SLOTS, rows].astype(F32)).astype(BF16)
            f_copy(c, k).start()
        for k in range(2):
            rows = pl.ds(pl.multiple_of(k * QUARTER + first[k] * EIGHTH, EIGHTH), EIGHTH)
            f_keep[c % SENDS, k] = own[c % 3, rows] + d_recv[c % SLOTS, rows].astype(F32)

    def r0_free(c, place):
        for k in range(2):
            f_copy(c, k).wait_send()

    def r1(c, place):
        for k in range(2):
            f_copy(c, k).wait_recv()
            for j in range(4):
                rows = pl.ds(j * PIECE, PIECE)
                zacc[c % ZSLOTS, j, k] = f_keep[c % SENDS, k, rows] + f_recv[c % SLOTS, k, rows].astype(F32)
        z_go(c, 1)

    def rz(s):
        def stage(c, place):
            for way in range(2):
                piece, ok = z_got(way, s)

                @pl.when(ok)
                def _():
                    z_copy(c, way, s).wait_recv()
                    zacc[c % ZSLOTS, piece] = (
                        zacc[c % ZSLOTS, piece] + z_recv[way, s - 1, c % SLOTS].astype(F32)
                    )

            if s < 3:
                z_go(c, s + 1)
                return
            for k in range(2):
                l_send[c % SENDS, k] = zacc[c % ZSLOTS, z, k].astype(BF16)
                l_copy(c, k).start()

        return stage

    def az_piece(way, s):
        piece = z - (s - 1) if way == 0 else z + (s - 1)
        ok = (z <= 2) & (piece >= 0) if way == 0 else (z >= 1) & (piece <= 3)
        return piece, ok

    def az_go(c, s, place):
        for way in range(2):
            piece, ok = az_piece(way, s)

            @pl.when(ok)
            def _():
                for k in range(2):
                    az_copy(c, way, s, k, piece, place).start()

    def az_free(s):
        def free(c, place):
            for way in range(2):
                piece, ok = az_piece(way, s)

                @pl.when(ok)
                def _():
                    for k in range(2):
                        az_copy(c, way, s, k, piece, place).wait_send()

        return free

    def l_go(c, place):
        for k in range(2):
            l_copy(c, k).wait_recv()
            y = (l_send[c % SENDS, k].astype(F32) + l_recv[c % SLOTS, k].astype(F32)).astype(BF16)
            y_buf[c % SENDS, k] = y
            if place == 0:
                y_local(c, k).start()
            else:
                piece_of(c, k, z, place)[...] = y
        az_go(c, 1, place)

    def l_free(c, place):
        for k in range(2):
            l_copy(c, k).wait_send()

    def az(s):
        def stage(c, place):
            for way in range(2):
                piece = z - s if way == 0 else z + s
                ok = piece >= 0 if way == 0 else piece <= 3

                @pl.when(ok)
                def _():
                    for k in range(2):
                        az_copy(c, way, s, k, piece, place).wait_recv()

            if s == 1 and place == 0:
                for k in range(2):
                    y_local(c, k).wait()
            if s < 3:
                az_go(c, s + 1, place)
                return
            for k in range(2):
                af_copy(c, k, first[k], place).start()

        return stage

    def af_free(c, place):
        for k in range(2):
            af_copy(c, k, first[k], place).wait_send()

    def a4(c, place):
        for k in range(2):
            af_copy(c, k, 1 - first[k], place).wait_recv()
        ad_copy(c, core, place).start()

    def a4_free(c, place):
        ad_copy(c, core, place).wait_send()

    def a5(c, place):
        ad_copy(c, 1 - core, place).wait_recv()

    stages = (
        (r0, r0_free, False),
        (r1, z_free(1), False),
        (rz(1), z_free(2), False),
        (rz(2), z_free(3), False),
        (rz(3), l_free, False),
        (l_go, az_free(1), True),
        (az(1), az_free(2), True),
        (az(2), az_free(3), True),
        (az(3), af_free, True),
        (a4, a4_free, True),
        (a5, None, True),
    )

    def at_place(c, ok, split, f):
        if not split:

            @pl.when(ok)
            def _():
                f(c, 0)

            return
        for place in range(2):

            @pl.when(ok & ((c < HBM_TILES) if place == 0 else (c >= HBM_TILES)))
            def _():
                f(c, place)

    def comm(u, part):
        for lag, (stage, free, split) in zip(LAG, stages):
            if lag % 2 != part:
                continue
            c = u - NK - lag // 2
            if free is not None:
                at_place(c - SENDS, (c >= SENDS) & (c < TILES + SENDS), split, free)
            at_place(c, (c >= 0) & (c < TILES), split, stage)

    def loads(u):
        p = u % 2
        rows = pl.ds(pl.multiple_of(lax.div(u, NK) * RB, RB), RB)
        deep = pl.ds(pl.multiple_of(lax.rem(u, NK) * KB, KB), KB)
        cols = pl.ds(pl.multiple_of(lax.rem(u, NC) * CB, CB), CB)
        up = (
            pltpu.make_async_copy(x.at[rows, deep], x_buf.at[p], load_sem.at[p, 0]),
            pltpu.make_async_copy(wg.at[deep], gu_buf.at[p, :, pl.ds(0, F)], load_sem.at[p, 1]),
            pltpu.make_async_copy(wu.at[deep], gu_buf.at[p, :, pl.ds(F, F)], load_sem.at[p, 2]),
        )
        down = pltpu.make_async_copy(wd.at[:, cols], wd_buf.at[p], load_sem.at[p, 3])
        return up, down

    def fetch(u):
        up, down = loads(u)

        @pl.when(u < TILES)
        def _():
            for copy in up:
                copy.start()

        @pl.when((u >= NK) & (u < NK + TILES))
        def _():
            down.start()

    acc[...] = jnp.zeros_like(acc)
    fetch(jnp.int32(0))

    def step(u, _):
        fetch(u + 1)
        up, down = loads(u)
        p = u % 2
        c = u - NK

        @pl.when((c >= SENDS) & (c < TILES + SENDS))
        def _():
            d_copy(c - SENDS).wait_send()

        @pl.when((c >= 0) & (c < TILES))
        def _():
            down.wait()
            term[...] = jnp.dot(hid[...], wd_buf[p], preferred_element_type=F32)
            d_send[c % SENDS] = term[pl.ds(pl.multiple_of((1 - core) * HALF, HALF), HALF)].astype(BF16)
            d_copy(c).start()
            own[c % 3] = term[pl.ds(pl.multiple_of(core * HALF, HALF), HALF)]

        comm(u, 0)

        @pl.when(u < TILES)
        def _():
            for copy in up:
                copy.wait()
            acc[...] += jnp.dot(x_buf[p], gu_buf[p], preferred_element_type=F32)

            @pl.when(lax.rem(u, NK) == NK - 1)
            def _():
                gate = acc[:, pl.ds(0, F)]
                hid[...] = (gate * jax.nn.sigmoid(gate) * acc[:, pl.ds(F, F)]).astype(BF16)
                acc[...] = jnp.zeros_like(acc)

        comm(u, 1)
        return 0

    lax.fori_loop(0, STEPS, step, 0)


def join(high, low, out, buf, in_sem, out_sem, low_sem):
    rows = HBM_ROWS // JOIN
    lows = pltpu.make_async_copy(low, out.at[pl.ds(HBM_ROWS, ROWS - HBM_ROWS)], low_sem)
    ins = [pltpu.make_async_copy(high.at[pl.ds(i * rows, rows)], buf.at[i], in_sem.at[i]) for i in range(JOIN)]
    outs = [pltpu.make_async_copy(buf.at[i], out.at[pl.ds(i * rows, rows)], out_sem.at[i]) for i in range(JOIN)]
    for copy in ins:
        copy.start()
    lows.start()
    for arrived, copy in zip(ins, outs):
        arrived.wait()
        copy.start()
    for copy in outs:
        copy.wait()
    lows.wait()


def block_of(x, wg, wu, wd):
    any_space = pl.BlockSpec(memory_space=pl.ANY)
    dma = pltpu.SemaphoreType.DMA
    high, low = pl.pallas_call(
        kernel,
        out_shape=(
            jax.ShapeDtypeStruct((HBM_ROWS, D), BF16),
            pltpu.VMEM((ROWS - HBM_ROWS, D), BF16),
        ),
        in_specs=[any_space] * 4,
        out_specs=(any_space, pl.BlockSpec(memory_space=pltpu.VMEM)),
        scratch_shapes=[
            pltpu.VMEM((2, RB, KB), BF16),
            pltpu.VMEM((2, KB, 2 * F), BF16),
            pltpu.VMEM((2, F, CB), BF16),
            pltpu.VMEM((RB, 2 * F), F32),
            pltpu.VMEM((RB, F), BF16),
            pltpu.VMEM((RB, CB), F32),
            pltpu.VMEM((3, HALF, CB), F32),
            pltpu.VMEM((SENDS, HALF, CB), BF16),
            pltpu.VMEM((SLOTS, HALF, CB), BF16),
            pltpu.VMEM((SENDS, 2, EIGHTH, CB), BF16),
            pltpu.VMEM((SENDS, 2, EIGHTH, CB), F32),
            pltpu.VMEM((SLOTS, 2, EIGHTH, CB), BF16),
            pltpu.VMEM((ZSLOTS, 4, 2, PIECE, CB), F32),
            pltpu.VMEM((2, 3, SENDS, 2, PIECE, CB), BF16),
            pltpu.VMEM((2, 3, SLOTS, 2, PIECE, CB), BF16),
            pltpu.VMEM((SENDS, 2, PIECE, CB), BF16),
            pltpu.VMEM((SLOTS, 2, PIECE, CB), BF16),
            pltpu.VMEM((SENDS, 2, PIECE, CB), BF16),
            dma((2, 4)),
            dma((SENDS,)), dma((SLOTS,)),
            dma((2, SENDS)), dma((2, SLOTS)),
            dma((6, SENDS)), dma((6, SLOTS)),
            dma((2, SENDS)), dma((2, SLOTS)),
            dma((2, SENDS)),
            dma((12, SENDS)), dma((12, SLOTS)),
            dma((2, SENDS)), dma((2, SLOTS)),
            dma((SENDS,)), dma((SLOTS,)),
        ],
        compiler_params=pltpu.CompilerParams(
            collective_id=0, has_side_effects=True, vmem_limit_bytes=40_000_000
        ),
    )(x, wg, wu, wd)
    low = pltpu.with_memory_space_constraint(low, pltpu.VMEM)
    return pl.pallas_call(
        join,
        out_shape=jax.ShapeDtypeStruct((ROWS, D), BF16),
        in_specs=[any_space] * 2,
        out_specs=any_space,
        scratch_shapes=[
            pltpu.VMEM((JOIN, HBM_ROWS // JOIN, D), BF16),
            dma((JOIN,)), dma((JOIN,)), dma,
        ],
        compiler_params=pltpu.CompilerParams(vmem_limit_bytes=24_000_000),
    )(high, low)


def solution(mesh):
    return jax.shard_map(
        block_of,
        mesh=mesh,
        in_specs=(P("dp", None), P(None, "tp"), P(None, "tp"), P("tp", None)),
        out_specs=P("dp", None),
        check_vma=False,
    )
```

```python
import jax
import jax.numpy as jnp
from jax import lax
from jax.experimental import pallas as pl
from jax.experimental.pallas import tpu as pltpu
from jax.sharding import PartitionSpec as P

MESH = pl.DeviceIdType.MESH
F32, BF16 = jnp.float32, jnp.bfloat16
ROWS, D, F = 2048, 8192, 896
RB, KB, CB = 256, 1024, 1024
NK, NC = D // KB, D // CB
TILES = (ROWS // RB) * NC
SLOTS = 24
SENDS = 4
ZSLOTS = 6
HBM_ROWS = 512
JOIN = 4
HBM_TILES = HBM_ROWS // RB * NC
HALF, QUARTER, EIGHTH, PIECE = RB // 2, RB // 4, RB // 8, RB // 32
LAG = (2, 5, 7, 10, 13, 16, 20, 23, 26, 38, 41)
STEPS = NK + TILES + SENDS + max(LAG) // 2 + 1


def kernel(
    x, wg, wu, wd, out_h, out_v,
    x_buf, gu_buf, wd_buf, acc, hid, term,
    own, d_send, d_recv, f_send, f_keep, f_recv, zacc, z_send, z_recv, l_send, l_recv, y_buf,
    load_sem, ds_sem, dr_sem, fs_sem, fr_sem, zs_sem, zr_sem, ls_sem, lr_sem, yl_sem,
    azs_sem, azr_sem, afs_sem, afr_sem, ads_sem, adr_sem,
):
    me = lax.axis_index("tp")
    core = lax.rem(me, 2)
    z = lax.rem(lax.div(me, 2), 4)
    yy = lax.rem(lax.div(me, 8), 2)
    xx = lax.div(me, 16)
    peer_core = me + 1 - 2 * core
    peer_x = me + 16 - 32 * xx
    peer_y = me + 8 - 16 * yy
    toward = (me + 2, me - 2)
    first = (xx, yy)
    first_peer, last_peer = (peer_x, peer_y), (peer_y, peer_x)

    barrier = pltpu.get_barrier_semaphore()

    def greet(device):
        pl.semaphore_signal(barrier, inc=1, device_id={"tp": device}, device_id_type=MESH)

    greet(peer_core)
    greet(peer_x)
    greet(peer_y)

    @pl.when(z < 3)
    def _():
        greet(me + 2)

    @pl.when(z > 0)
    def _():
        greet(me - 2)

    greeted = 3 + jnp.where(z < 3, 1, 0) + jnp.where(z > 0, 1, 0)

    def remote(src, dst, send_sem, recv_sem, device):
        return pltpu.make_async_remote_copy(
            src_ref=src, dst_ref=dst, send_sem=send_sem, recv_sem=recv_sem,
            device_id={"tp": device}, device_id_type=MESH,
        )

    def block(c, row, rows, place):
        ref, base = ((out_h, 0), (out_v, HBM_ROWS))[place]
        start = pl.multiple_of(lax.div(c, NC) * RB - base + row, PIECE)
        return ref.at[pl.ds(start, rows), pl.ds(pl.multiple_of(lax.rem(c, NC) * CB, CB), CB)]

    def d_copy(c):
        return remote(d_send.at[c % SENDS], d_recv.at[c % SLOTS], ds_sem.at[c % SENDS], dr_sem.at[c % SLOTS], peer_core)

    def f_copy(c, k):
        return remote(
            f_send.at[c % SENDS, k], f_recv.at[c % SLOTS, k], fs_sem.at[k, c % SENDS], fr_sem.at[k, c % SLOTS], first_peer[k]
        )

    def z_copy(c, way, s):
        return remote(
            z_send.at[way, s - 1, c % SENDS], z_recv.at[way, s - 1, c % SLOTS],
            zs_sem.at[way * 3 + s - 1, c % SENDS], zr_sem.at[way * 3 + s - 1, c % SLOTS], toward[way],
        )

    def l_copy(c, k):
        return remote(
            l_send.at[c % SENDS, k], l_recv.at[c % SLOTS, k], ls_sem.at[k, c % SENDS], lr_sem.at[k, c % SLOTS], last_peer[k]
        )

    def piece_of(c, k, piece, place):
        return block(c, core * HALF + k * QUARTER + first[k] * EIGHTH + piece * PIECE, PIECE, place)

    def y_local(c, k):
        return pltpu.make_async_copy(y_buf.at[c % SENDS, k], piece_of(c, k, z, 0), yl_sem.at[k, c % SENDS])

    def az_copy(c, way, s, k, piece, place):
        rows = piece_of(c, k, piece, place)
        i = (way * 3 + s - 1) * 2 + k
        src = y_buf.at[c % SENDS, k] if s == 1 else rows
        return remote(src, rows, azs_sem.at[i, c % SENDS], azr_sem.at[i, c % SLOTS], toward[way])

    def af_copy(c, k, half, place):
        rows = block(c, core * HALF + k * QUARTER + half * EIGHTH, EIGHTH, place)
        return remote(rows, rows, afs_sem.at[k, c % SENDS], afr_sem.at[k, c % SLOTS], first_peer[k])

    def ad_copy(c, half, place):
        rows = block(c, half * HALF, HALF, place)
        return remote(rows, rows, ads_sem.at[c % SENDS], adr_sem.at[c % SLOTS], peer_core)

    def z_piece(way, s):
        piece = 4 - s + z if way == 0 else z + s - 4
        ok = (z <= 2) & (piece <= 3) if way == 0 else (z >= 1) & (piece >= 0)
        return piece, ok

    def z_got(way, s):
        piece = 3 - s + z if way == 0 else z + s - 3
        ok = (z >= 1) & (piece <= 3) if way == 0 else (z <= 2) & (piece >= 0)
        return piece, ok

    def z_go(c, s):
        for way in range(2):
            piece, ok = z_piece(way, s)

            @pl.when(ok)
            def _():
                z_send[way, s - 1, c % SENDS] = zacc[c % ZSLOTS, piece].astype(BF16)
                z_copy(c, way, s).start()

    def z_free(s):
        def free(c, place):
            for way in range(2):
                piece, ok = z_piece(way, s)

                @pl.when(ok)
                def _():
                    z_copy(c, way, s).wait_send()

        return free

    def r0(c, place):
        d_copy(c).wait_recv()
        for k in range(2):
            rows = pl.ds(pl.multiple_of(k * QUARTER + (1 - first[k]) * EIGHTH, EIGHTH), EIGHTH)
            f_send[c % SENDS, k] = (own[c % 3, rows] + d_recv[c % SLOTS, rows].astype(F32)).astype(BF16)
            f_copy(c, k).start()
        for k in range(2):
            rows = pl.ds(pl.multiple_of(k * QUARTER + first[k] * EIGHTH, EIGHTH), EIGHTH)
            f_keep[c % SENDS, k] = own[c % 3, rows] + d_recv[c % SLOTS, rows].astype(F32)

    def r0_free(c, place):
        for k in range(2):
            f_copy(c, k).wait_send()

    def r1(c, place):
        for k in range(2):
            f_copy(c, k).wait_recv()
            for j in range(4):
                rows = pl.ds(j * PIECE, PIECE)
                zacc[c % ZSLOTS, j, k] = f_keep[c % SENDS, k, rows] + f_recv[c % SLOTS, k, rows].astype(F32)
        z_go(c, 1)

    def rz(s):
        def stage(c, place):
            for way in range(2):
                piece, ok = z_got(way, s)

                @pl.when(ok)
                def _():
                    z_copy(c, way, s).wait_recv()
                    zacc[c % ZSLOTS, piece] = (
                        zacc[c % ZSLOTS, piece] + z_recv[way, s - 1, c % SLOTS].astype(F32)
                    )

            if s < 3:
                z_go(c, s + 1)
                return
            for k in range(2):
                l_send[c % SENDS, k] = zacc[c % ZSLOTS, z, k].astype(BF16)
                l_copy(c, k).start()

        return stage

    def az_piece(way, s):
        piece = z - (s - 1) if way == 0 else z + (s - 1)
        ok = (z <= 2) & (piece >= 0) if way == 0 else (z >= 1) & (piece <= 3)
        return piece, ok

    def az_go(c, s, place):
        for way in range(2):
            piece, ok = az_piece(way, s)

            @pl.when(ok)
            def _():
                for k in range(2):
                    az_copy(c, way, s, k, piece, place).start()

    def az_free(s):
        def free(c, place):
            for way in range(2):
                piece, ok = az_piece(way, s)

                @pl.when(ok)
                def _():
                    for k in range(2):
                        az_copy(c, way, s, k, piece, place).wait_send()

        return free

    def l_go(c, place):
        for k in range(2):
            l_copy(c, k).wait_recv()
            y = (l_send[c % SENDS, k].astype(F32) + l_recv[c % SLOTS, k].astype(F32)).astype(BF16)
            y_buf[c % SENDS, k] = y
            if place == 0:
                y_local(c, k).start()
            else:
                piece_of(c, k, z, place)[...] = y
        az_go(c, 1, place)

    def l_free(c, place):
        for k in range(2):
            l_copy(c, k).wait_send()

    def az(s):
        def stage(c, place):
            for way in range(2):
                piece = z - s if way == 0 else z + s
                ok = piece >= 0 if way == 0 else piece <= 3

                @pl.when(ok)
                def _():
                    for k in range(2):
                        az_copy(c, way, s, k, piece, place).wait_recv()

            if s == 1 and place == 0:
                for k in range(2):
                    y_local(c, k).wait()
            if s < 3:
                az_go(c, s + 1, place)
                return
            for k in range(2):
                af_copy(c, k, first[k], place).start()

        return stage

    def af_free(c, place):
        for k in range(2):
            af_copy(c, k, first[k], place).wait_send()

    def a4(c, place):
        for k in range(2):
            af_copy(c, k, 1 - first[k], place).wait_recv()
        ad_copy(c, core, place).start()

    def a4_free(c, place):
        ad_copy(c, core, place).wait_send()

    def a5(c, place):
        ad_copy(c, 1 - core, place).wait_recv()

    stages = (
        (r0, r0_free, False),
        (r1, z_free(1), False),
        (rz(1), z_free(2), False),
        (rz(2), z_free(3), False),
        (rz(3), l_free, False),
        (l_go, az_free(1), True),
        (az(1), az_free(2), True),
        (az(2), az_free(3), True),
        (az(3), af_free, True),
        (a4, a4_free, True),
        (a5, None, True),
    )

    def at_place(c, ok, split, f):
        if not split:

            @pl.when(ok)
            def _():
                f(c, 0)

            return
        for place in range(2):

            @pl.when(ok & ((c < HBM_TILES) if place == 0 else (c >= HBM_TILES)))
            def _():
                f(c, place)

    def comm(u, part):
        for lag, (stage, free, split) in zip(LAG, stages):
            if lag % 2 != part:
                continue
            c = u - NK - lag // 2
            if free is not None:
                at_place(c - SENDS, (c >= SENDS) & (c < TILES + SENDS), split, free)
            at_place(c, (c >= 0) & (c < TILES), split, stage)

    def loads(u):
        p = u % 2
        rows = pl.ds(pl.multiple_of(lax.div(u, NK) * RB, RB), RB)
        deep = pl.ds(pl.multiple_of(lax.rem(u, NK) * KB, KB), KB)
        cols = pl.ds(pl.multiple_of(lax.rem(u, NC) * CB, CB), CB)
        up = (
            pltpu.make_async_copy(x.at[rows, deep], x_buf.at[p], load_sem.at[p, 0]),
            pltpu.make_async_copy(wg.at[deep], gu_buf.at[p, :, pl.ds(0, F)], load_sem.at[p, 1]),
            pltpu.make_async_copy(wu.at[deep], gu_buf.at[p, :, pl.ds(F, F)], load_sem.at[p, 2]),
        )
        down = pltpu.make_async_copy(wd.at[:, cols], wd_buf.at[p], load_sem.at[p, 3])
        return up, down

    def fetch(u):
        up, down = loads(u)

        @pl.when(u < TILES)
        def _():
            for copy in up:
                copy.start()

        @pl.when((u >= NK) & (u < NK + TILES))
        def _():
            down.start()

    acc[...] = jnp.zeros_like(acc)
    fetch(jnp.int32(0))

    def step(u, _):
        fetch(u + 1)
        up, down = loads(u)
        p = u % 2
        c = u - NK

        @pl.when(c == 0)
        def _():
            pl.semaphore_wait(barrier, greeted)

        @pl.when((c >= SENDS) & (c < TILES + SENDS))
        def _():
            d_copy(c - SENDS).wait_send()

        @pl.when((c >= 0) & (c < TILES))
        def _():
            down.wait()
            term[...] = jnp.dot(hid[...], wd_buf[p], preferred_element_type=F32)
            d_send[c % SENDS] = term[pl.ds(pl.multiple_of((1 - core) * HALF, HALF), HALF)].astype(BF16)
            d_copy(c).start()
            own[c % 3] = term[pl.ds(pl.multiple_of(core * HALF, HALF), HALF)]

        comm(u, 0)

        @pl.when(u < TILES)
        def _():
            for copy in up:
                copy.wait()
            acc[...] += jnp.dot(x_buf[p], gu_buf[p], preferred_element_type=F32)

            @pl.when(lax.rem(u, NK) == NK - 1)
            def _():
                gate = acc[:, pl.ds(0, F)]
                hid[...] = (gate * jax.nn.sigmoid(gate) * acc[:, pl.ds(F, F)]).astype(BF16)
                acc[...] = jnp.zeros_like(acc)

        comm(u, 1)
        return 0

    lax.fori_loop(0, STEPS, step, 0)


def join(high, low, out, buf, in_sem, out_sem, low_sem):
    rows = HBM_ROWS // JOIN
    lows = pltpu.make_async_copy(low, out.at[pl.ds(HBM_ROWS, ROWS - HBM_ROWS)], low_sem)
    ins = [pltpu.make_async_copy(high.at[pl.ds(i * rows, rows)], buf.at[i], in_sem.at[i]) for i in range(JOIN)]
    outs = [pltpu.make_async_copy(buf.at[i], out.at[pl.ds(i * rows, rows)], out_sem.at[i]) for i in range(JOIN)]
    for copy in ins:
        copy.start()
    lows.start()
    for arrived, copy in zip(ins, outs):
        arrived.wait()
        copy.start()
    for copy in outs:
        copy.wait()
    lows.wait()


def block_of(x, wg, wu, wd):
    any_space = pl.BlockSpec(memory_space=pl.ANY)
    dma = pltpu.SemaphoreType.DMA
    high, low = pl.pallas_call(
        kernel,
        out_shape=(
            jax.ShapeDtypeStruct((HBM_ROWS, D), BF16),
            pltpu.VMEM((ROWS - HBM_ROWS, D), BF16),
        ),
        in_specs=[any_space] * 4,
        out_specs=(any_space, pl.BlockSpec(memory_space=pltpu.VMEM)),
        scratch_shapes=[
            pltpu.VMEM((2, RB, KB), BF16),
            pltpu.VMEM((2, KB, 2 * F), BF16),
            pltpu.VMEM((2, F, CB), BF16),
            pltpu.VMEM((RB, 2 * F), F32),
            pltpu.VMEM((RB, F), BF16),
            pltpu.VMEM((RB, CB), F32),
            pltpu.VMEM((3, HALF, CB), F32),
            pltpu.VMEM((SENDS, HALF, CB), BF16),
            pltpu.VMEM((SLOTS, HALF, CB), BF16),
            pltpu.VMEM((SENDS, 2, EIGHTH, CB), BF16),
            pltpu.VMEM((SENDS, 2, EIGHTH, CB), F32),
            pltpu.VMEM((SLOTS, 2, EIGHTH, CB), BF16),
            pltpu.VMEM((ZSLOTS, 4, 2, PIECE, CB), F32),
            pltpu.VMEM((2, 3, SENDS, 2, PIECE, CB), BF16),
            pltpu.VMEM((2, 3, SLOTS, 2, PIECE, CB), BF16),
            pltpu.VMEM((SENDS, 2, PIECE, CB), BF16),
            pltpu.VMEM((SLOTS, 2, PIECE, CB), BF16),
            pltpu.VMEM((SENDS, 2, PIECE, CB), BF16),
            dma((2, 4)),
            dma((SENDS,)), dma((SLOTS,)),
            dma((2, SENDS)), dma((2, SLOTS)),
            dma((6, SENDS)), dma((6, SLOTS)),
            dma((2, SENDS)), dma((2, SLOTS)),
            dma((2, SENDS)),
            dma((12, SENDS)), dma((12, SLOTS)),
            dma((2, SENDS)), dma((2, SLOTS)),
            dma((SENDS,)), dma((SLOTS,)),
        ],
        compiler_params=pltpu.CompilerParams(
            collective_id=0, has_side_effects=True, vmem_limit_bytes=40_000_000
        ),
    )(x, wg, wu, wd)
    low = pltpu.with_memory_space_constraint(low, pltpu.VMEM)
    return pl.pallas_call(
        join,
        out_shape=jax.ShapeDtypeStruct((ROWS, D), BF16),
        in_specs=[any_space] * 2,
        out_specs=any_space,
        scratch_shapes=[
            pltpu.VMEM((JOIN, HBM_ROWS // JOIN, D), BF16),
            dma((JOIN,)), dma((JOIN,)), dma,
        ],
        compiler_params=pltpu.CompilerParams(vmem_limit_bytes=24_000_000),
    )(high, low)


def solution(mesh):
    return jax.shard_map(
        block_of,
        mesh=mesh,
        in_specs=(P("dp", None), P(None, "tp"), P(None, "tp"), P("tp", None)),
        out_specs=P("dp", None),
        check_vma=False,
    )
```
